8 devices in a mesh: dp: 1 (over z), tp: 8 (over x, y, core).
Axes of the slice: x: 2, y: 2, z: 1, core: 2. Of those that a mesh axis runs over, the one named last changes fastest.
Arguments:
- x: bfloat16 [64, 5120], P('dp')
- k_cache: bfloat16 [64, 4096, 8, 128], P('dp', None, 'tp')
- v_cache: bfloat16 [64, 4096, 8, 128], P('dp', None, 'tp')
- gain_a: bfloat16 [5120], replicated
- wq: bfloat16 [5120, 4096], P(None, 'tp')
- wo: bfloat16 [4096, 5120], P('tp')
- gain_m: bfloat16 [5120], replicated
- w_gate: bfloat16 [5120, 32768], P(None, 'tp')
- w_up: bfloat16 [5120, 32768], P(None, 'tp')
- w_down: bfloat16 [32768, 5120], P('tp')
Outputs:
- output: bfloat16 [64, 5120], P('dp')
All inputs are finite; a program needn't handle non-finite values.
Results may differ from the reference program's by a relative error of at most 0.017.
Values are sent between devices in bfloat16 or wider.
A program may use at most 2 GiB of HBM per device.

```python
import jax
import jax.numpy as jnp
from jax import lax

BATCH = 64
CACHE = 4096
D = 5120
HEADS = 32
KV_HEADS = 8
HEAD = 128
FF = 32768
THETA = 10000


def setup_inputs(seed: int = 0, part: int = 0) -> dict:
    kx, kc, kw, kn, kq, ko, km, kg, ku, kd = jax.random.split(jax.random.key(seed), 10)
    kx, kc, kw = (jax.random.fold_in(k, part) for k in (kx, kc, kw))

    def weights(key, rows, columns):
        return jax.random.normal(key, (rows, columns), jnp.float32) * rows**-0.5

    drawn = {
        "x": jax.random.normal(kx, (BATCH, D), jnp.float32),
        "k_cache": 2 * jax.random.normal(kc, (BATCH, CACHE, KV_HEADS, HEAD), jnp.float32),
        "v_cache": 4 * jax.random.normal(kw, (BATCH, CACHE, KV_HEADS, HEAD), jnp.float32),
        "gain_a": 1 + 0.1 * jax.random.normal(kn, (D,), jnp.float32),
        "wq": 2 * weights(kq, D, HEADS * HEAD),
        "wo": weights(ko, HEADS * HEAD, D),
        "gain_m": 1 + 0.1 * jax.random.normal(km, (D,), jnp.float32),
        "w_gate": weights(kg, D, FF),
        "w_up": weights(ku, D, FF),
        "w_down": 2 * weights(kd, FF, D),
    }
    return {k: v.astype(jnp.bfloat16) for k, v in drawn.items()}


def normed(x, gain):
    wide = x.astype(jnp.float32)
    scale = lax.rsqrt(jnp.mean(wide * wide, -1, keepdims=True) + 1e-6)
    return (wide * scale * gain.astype(jnp.float32)).astype(jnp.bfloat16)


def turned(t, place, theta):
    half = t.shape[-1] // 2
    angle = place.astype(jnp.float32)[:, None] * theta ** (-jnp.arange(half, dtype=jnp.float32) / half)
    cos, sin = jnp.cos(angle)[:, None], jnp.sin(angle)[:, None]
    a, b = t[..., :half].astype(jnp.float32), t[..., half:].astype(jnp.float32)
    return jnp.concatenate([a * cos - b * sin, b * cos + a * sin], -1).astype(jnp.bfloat16)


def matmul(a, w):
    return jnp.dot(a, w, preferred_element_type=jnp.float32).astype(jnp.bfloat16)


def einsum(form, a, b):
    return jnp.einsum(form, a.astype(jnp.float32), b.astype(jnp.float32))


def seen_by(a, wq, k_cache, v_cache, head, theta):
    batch, cache, kv_heads = k_cache.shape[:3]
    place = jnp.full((batch,), cache - 1)
    q = turned(matmul(a, wq).reshape(batch, -1, head), place, theta).reshape(batch, kv_heads, -1, head)
    scores = einsum("bgsd,bugd->bgsu", q, k_cache) * head**-0.5
    weights = jax.nn.softmax(scores, -1).astype(jnp.bfloat16)
    return einsum("bgsu,bugd->bgsd", weights, v_cache).astype(jnp.bfloat16).reshape(batch, -1)


def hidden_of(b, w_gate, w_up):
    gate = jnp.dot(b, w_gate, preferred_element_type=jnp.float32)
    up = jnp.dot(b, w_up, preferred_element_type=jnp.float32)
    return (jax.nn.silu(gate) * up).astype(jnp.bfloat16)


def reference(x, k_cache, v_cache, gain_a, wq, wo, gain_m, w_gate, w_up, w_down):
    seen = seen_by(normed(x, gain_a), wq, k_cache, v_cache, HEAD, THETA)
    h = (x.astype(jnp.float32) + jnp.dot(seen, wo, preferred_element_type=jnp.float32)).astype(jnp.bfloat16)
    hidden = hidden_of(normed(h, gain_m), w_gate, w_up)
    return (h.astype(jnp.float32) + jnp.dot(hidden, w_down, preferred_element_type=jnp.float32)).astype(jnp.bfloat16)
```

```python
import functools

import jax
import jax.numpy as jnp
import numpy as np
from jax import lax
from jax.experimental import pallas as pl
from jax.experimental.pallas import tpu as pltpu
from jax.sharding import PartitionSpec as P

BATCH = 64
CACHE = 4096
D = 5120
HEAD = 128
GROUP = 4
FF = 4096
THETA = 10000
DEV = 8
MESH = pl.DeviceIdType.MESH

PAIRS = BATCH // 2
RING = 4
SLOTS = 7
WIDE = 256
GU_STEPS = FF // WIDE
DN_STEPS = D // (2 * WIDE)
SUBS = D // WIDE
CHUNK = 16
CHUNKS = BATCH // CHUNK
STEPS = PAIRS // 2
SPC = CHUNK // 4
OWN = D // DEV
KEYS = 256
LAG = 4
LOG2E = 1.4426950408889634
F32, BF16 = jnp.float32, jnp.bfloat16


def rotary():
    half = HEAD // 2
    angle = (CACHE - 1) * np.float64(THETA) ** (-np.arange(half) / half)
    cos, sin = np.cos(angle), np.sin(angle)
    return np.stack([np.concatenate([cos, cos]), np.concatenate([-sin, sin])]).astype(np.float32)


def norm_rows(src, gain_ref, dst):
    step = 512
    total = jnp.zeros((16, 128), F32)
    for c in range(D // step):
        t = src(c * step, step).astype(F32)
        t = t * t
        for j in range(step // 128):
            total = total + t[:, j * 128 : (j + 1) * 128]
    scale = lax.rsqrt(jnp.sum(total, axis=1, keepdims=True) * (1.0 / D) + 1e-6)
    for c in range(D // step):
        t = src(c * step, step).astype(F32)
        dst(c * step, step, (t * scale * gain_ref[:, c * step : (c + 1) * step].astype(F32)).astype(BF16))


def kernel(
    x_hbm, k_hbm, v_hbm, ga_ref, rot_ref, wq_hbm, wo_hbm, gm_ref, wg_hbm, wu_hbm, wd_hbm, y_hbm,
    kbuf, vbuf, wbuf, wobuf, xbuf, abuf, hbuf, hid, qs, os, prob,
    rs_send, rs_own, rs_recv, y_send, y_own, y_recv, ybuf,
    x_sem, k_sem, v_sem, w_sem, wo_sem, out_sem,
    rs_ssem, rs_rsem, ag_ssem, ag_rsem, ys_ssem, ys_rsem, yg_ssem, yg_rsem,
):
    me = lax.axis_index("tp")
    chip, core = me // 2, me % 2

    def k_copy(i):
        return pltpu.make_async_copy(k_hbm.at[pl.ds(2 * i, 2)], kbuf.at[i % RING], k_sem.at[i % RING])

    def v_copy(i):
        return pltpu.make_async_copy(v_hbm.at[pl.ds(2 * i, 2)], vbuf.at[i % RING], v_sem.at[i % RING])

    def gu_copy(j, half):
        cols = pl.ds(pl.multiple_of(j * WIDE, WIDE), WIDE)
        return pltpu.make_async_copy((wg_hbm, wu_hbm)[half].at[:, cols], wbuf.at[j % SLOTS, half], w_sem.at[j % SLOTS, half])

    def dn_copy(j, half):
        cols = pl.ds(pl.multiple_of((j - GU_STEPS) * 2 * WIDE + half * WIDE, WIDE), WIDE)
        return pltpu.make_async_copy(wd_hbm.at[:, cols], wbuf.at[j % SLOTS, half, pl.ds(0, FF)], w_sem.at[j % SLOTS, half])

    def gu_start(j):
        gu_copy(j, 0).start()
        gu_copy(j, 1).start()

    def dn_start(j):
        dn_copy(j, 0).start()
        dn_copy(j, 1).start()

    def wq_copy(half):
        return pltpu.make_async_copy(
            wq_hbm.at[:, pl.ds(half * WIDE, WIDE)], wbuf.at[SLOTS - 1, half], w_sem.at[SLOTS - 1, half]
        )

    x_copy = pltpu.make_async_copy(x_hbm, xbuf, x_sem)
    wo_copy = pltpu.make_async_copy(wo_hbm, wobuf, wo_sem)
    x_copy.start()
    wq_copy(0).start()
    wq_copy(1).start()
    for i in range(RING):
        k_copy(i).start()
        v_copy(i).start()
    wo_copy.start()
    gu_start(0)

    barrier = pltpu.get_barrier_semaphore()
    for o in range(1, DEV):
        pl.semaphore_signal(barrier, inc=1, device_id={"tp": lax.rem(me + o, DEV)}, device_id_type=MESH)

    x_copy.wait()

    @pl.loop(0, BATCH // 16)
    def _(r):
        rows = pl.ds(pl.multiple_of(r * 16, 16), 16)

        def dst(c, n, v):
            abuf[rows, c : c + n] = v

        norm_rows(lambda c, n: xbuf[rows, c : c + n], ga_ref, dst)

    cos, sin = rot_ref[0:1, :], rot_ref[1:2, :]
    for half in range(2):
        wq_copy(half).wait()
        q = jnp.dot(abuf[...], wbuf[SLOTS - 1, half], preferred_element_type=F32).astype(BF16).astype(F32)
        for g in range(2):
            t = q[:, g * HEAD : (g + 1) * HEAD]
            t = t * cos + pltpu.roll(t, HEAD // 2, 1) * sin
            qs[pl.ds(2 * half + g, BATCH, stride=GROUP), :] = t.astype(BF16).astype(F32)

    pl.semaphore_wait(barrier, DEV - 1)

    upper = lax.broadcasted_iota(jnp.int32, (8, HEAD), 0) < GROUP

    def scores(i):
        slot = i % RING
        q = qs[pl.ds(pl.multiple_of(i * 8, 8), 8), :]
        q = jnp.concatenate([jnp.where(upper, q, 0.0), jnp.where(upper, 0.0, q)], axis=1).astype(BF16)
        parts = []
        for u in range(CACHE // KEYS):
            keys = slice(u * KEYS, (u + 1) * KEYS)
            k = jnp.concatenate([kbuf[slot, 0, keys, :], kbuf[slot, 1, keys, :]], axis=1)
            parts.append(
                lax.dot_general(q, k, (((1,), (1,)), ((), ())), preferred_element_type=F32) * (HEAD**-0.5 * LOG2E)
            )
        top = functools.reduce(jnp.maximum, parts)
        top = jnp.max(top, axis=1, keepdims=True)
        parts = [jnp.exp2(t - top) for t in parts]
        total = functools.reduce(jnp.add, parts)
        inverse = 1.0 / jnp.sum(total, axis=1, keepdims=True)
        for u, t in enumerate(parts):
            prob[i % 4, :, u * KEYS : (u + 1) * KEYS] = (t * inverse).astype(BF16)

    def mix(i):
        slot = i % RING
        out = jnp.zeros((8, 2 * HEAD), F32)
        for u in range(CACHE // KEYS):
            keys = slice(u * KEYS, (u + 1) * KEYS)
            v = jnp.concatenate([vbuf[slot, 0, keys, :], vbuf[slot, 1, keys, :]], axis=1)
            out = out + jnp.dot(prob[i % 4, :, keys], v, preferred_element_type=F32)
        os[pl.ds(pl.multiple_of(i * 8, 8), 8), :] = jnp.where(upper, out[:, :HEAD], out[:, HEAD:])

    def own_cols(d):
        return pl.ds(pl.multiple_of(d * OWN, 128), OWN)

    def rs_copy(c, o):
        return pltpu.make_async_remote_copy(
            src_ref=rs_send.at[c, o - 1], dst_ref=rs_recv.at[c, o - 1], send_sem=rs_ssem.at[c], recv_sem=rs_rsem.at[c],
            device_id={"tp": lax.rem(me + o, DEV)}, device_id_type=MESH,
        )

    def ag_copy(c, o):
        return pltpu.make_async_remote_copy(
            src_ref=hbuf.at[c, :, own_cols(me)], dst_ref=hbuf.at[c, :, own_cols(me)], send_sem=ag_ssem.at[c],
            recv_sem=ag_rsem.at[c], device_id={"tp": lax.rem(me + o, DEV)}, device_id_type=MESH,
        )

    def all_of(ref, sem):
        return pltpu.make_async_copy(ref, ref, sem)

    def h_terms(c):
        seen = jnp.concatenate(
            [os[pl.ds(c * CHUNK * GROUP + g, CHUNK, stride=GROUP), :] for g in range(GROUP)], axis=1
        ).astype(BF16)
        for o in list(range(1, DEV)) + [0]:
            t = jnp.dot(seen, wobuf[:, own_cols(lax.rem(me + o, DEV))], preferred_element_type=F32)
            if o:
                rs_send[c, o - 1] = t.astype(BF16)
                rs_copy(c, o).start()
            else:
                rs_own[c] = t

    def h_sum(c):
        all_of(rs_recv.at[c], rs_rsem.at[c]).wait()
        rows = pl.ds(pl.multiple_of(c * CHUNK, CHUNK), CHUNK)
        t = rs_own[c]
        for o in range(DEV - 1):
            t = t + rs_recv[c, o].astype(F32)
        hbuf[c, :, own_cols(me)] = (xbuf[rows, own_cols(me)].astype(F32) + t).astype(BF16)
        for o in range(1, DEV):
            ag_copy(c, o).start()

    def h_norm(c):
        all_of(rs_recv.at[c], ag_rsem.at[c]).wait()
        rows = pl.ds(pl.multiple_of(c * CHUNK, CHUNK), CHUNK)

        def dst(at, n, v):
            abuf[rows, at : at + n] = v

        norm_rows(lambda at, n: hbuf[c, :, at : at + n], gm_ref, dst)

    for p in range(2):
        k_copy(p).wait()
    for p in range(2):
        scores(p)
    for p in range(2):
        k_copy(RING + p).start()

    @pl.loop(1, STEPS)
    def _(i):
        for p in range(2):
            k_copy(2 * i + p).wait()
            v_copy(2 * i - 2 + p).wait()
        for p in range(2):
            scores(2 * i + p)
        for p in range(2):
            mix(2 * i - 2 + p)

        @pl.when(2 * i + RING < PAIRS)
        def _():
            for p in range(2):
                k_copy(2 * i + RING + p).start()

        @pl.when(2 * i - 2 + RING < PAIRS)
        def _():
            for p in range(2):
                v_copy(2 * i - 2 + RING + p).start()

        @pl.when(i >= STEPS - 2)
        def _():
            gu_start(i - STEPS + 3)

        @pl.when(i == SPC)
        def _():
            wo_copy.wait()

        @pl.when((i % SPC == 0) & (i >= SPC))
        def _():
            h_terms(i // SPC - 1)

        @pl.when((i % SPC == 1) & (i >= SPC))
        def _():
            h_sum(i // SPC - 1)

        @pl.when((i % SPC == 2) & (i >= SPC))
        def _():
            h_norm(i // SPC - 1)

    for p in range(2):
        v_copy(PAIRS - 2 + p).wait()
    for p in range(2):
        mix(PAIRS - 2 + p)
    for j in range(3, SLOTS):
        gu_start(j)
    h_terms(CHUNKS - 1)
    h_sum(CHUNKS - 1)
    h_norm(CHUNKS - 1)

    @pl.loop(0, GU_STEPS)
    def _(j):
        slot = j % SLOTS
        gu_copy(j, 0).wait()
        gu_copy(j, 1).wait()
        b = abuf[...]
        gate = jnp.dot(b, wbuf[slot, 0], preferred_element_type=F32)
        up = jnp.dot(b, wbuf[slot, 1], preferred_element_type=F32)
        hid[:, pl.ds(pl.multiple_of(j * WIDE, WIDE), WIDE)] = (jax.nn.silu(gate) * up).astype(BF16)

        @pl.when(j + SLOTS < GU_STEPS)
        def _():
            gu_start(j + SLOTS)

        @pl.when(j + SLOTS >= GU_STEPS)
        def _():
            dn_start(j + SLOTS)

    def y_place(m, d):
        return (
            pl.ds(pl.multiple_of((d // 2) * 16, 16), 16),
            pl.ds(pl.multiple_of(m * WIDE + (d % 2) * 128, 128), 128),
        )

    def ys_copy(m, o):
        d = lax.rem(me + o, DEV)
        return pltpu.make_async_remote_copy(
            src_ref=y_send.at[m, d], dst_ref=y_recv.at[m, o - 1], send_sem=ys_ssem, recv_sem=ys_rsem.at[m],
            device_id={"tp": d}, device_id_type=MESH,
        )

    def yg_copy(m, o):
        rows, cols = y_place(m, me)
        return pltpu.make_async_remote_copy(
            src_ref=ybuf.at[rows, cols], dst_ref=ybuf.at[rows, cols], send_sem=yg_ssem, recv_sem=yg_rsem.at[m],
            device_id={"tp": lax.rem(me + o, DEV)}, device_id_type=MESH,
        )

    def y_sum(m):
        all_of(y_recv.at[m], ys_rsem.at[m]).wait()
        rows, cols = y_place(m, me)
        t = y_own[m % (LAG + 1), me]
        for o in range(DEV - 1):
            t = t + y_recv[m, o].astype(F32)
        ybuf[rows, cols] = (hbuf[chip, :, cols].astype(F32) + t).astype(BF16)
        for o in range(1, DEV):
            yg_copy(m, o).start()

    @pl.loop(0, SUBS)
    def _(m):
        j, half = GU_STEPS + m // 2, m % 2
        slot = j % SLOTS
        pltpu.make_async_copy(wd_hbm.at[:, pl.ds(0, WIDE)], wbuf.at[slot, half, pl.ds(0, FF)], w_sem.at[slot, half]).wait()
        t = jnp.dot(hid[...], wbuf[slot, half, :FF], preferred_element_type=F32)
        for d in range(DEV):
            part = t[(d // 2) * 16 : (d // 2) * 16 + 16, (d % 2) * 128 : (d % 2) * 128 + 128]
            y_own[m % (LAG + 1), d] = part
            y_send[m, d] = part.astype(BF16)
        for o in range(1, DEV):
            ys_copy(m, o).start()

        @pl.when((half == 1) & (j + SLOTS < GU_STEPS + DN_STEPS))
        def _():
            dn_start(j + SLOTS)

        @pl.when(m >= LAG)
        def _():
            y_sum(m - LAG)

    @pl.loop(SUBS - LAG, SUBS)
    def _(m):
        y_sum(m)

    @pl.loop(0, SUBS)
    def _(m):
        all_of(y_recv.at[m], yg_rsem.at[m]).wait()

    out = pltpu.make_async_copy(ybuf, y_hbm, out_sem)
    out.start()

    for c in range(CHUNKS):
        all_of(rs_recv.at[c], rs_ssem.at[c]).wait()
        all_of(rs_recv.at[c], ag_ssem.at[c]).wait()
    all_of(y_recv, ys_ssem).wait()
    all_of(y_recv, yg_ssem).wait()
    out.wait()


def solution(mesh):
    def step(x, k_cache, v_cache, gain_a, wq, wo, gain_m, w_gate, w_up, w_down):
        hbm = pl.BlockSpec(memory_space=pltpu.HBM)
        vmem = pl.BlockSpec(memory_space=pltpu.VMEM)
        dma = pltpu.SemaphoreType.DMA
        return pl.pallas_call(
            kernel,
            out_shape=jax.ShapeDtypeStruct((BATCH, D), BF16),
            in_specs=[hbm, hbm, hbm, vmem, vmem, hbm, hbm, vmem, hbm, hbm, hbm],
            out_specs=hbm,
            scratch_shapes=[
                pltpu.VMEM((RING, 2, CACHE, HEAD), BF16),
                pltpu.VMEM((RING, 2, CACHE, HEAD), BF16),
                pltpu.VMEM((SLOTS, 2, D, WIDE), BF16),
                pltpu.VMEM((GROUP * HEAD, D), BF16),
                pltpu.VMEM((BATCH, D), BF16),
                pltpu.VMEM((BATCH, D), BF16),
                pltpu.VMEM((CHUNKS, CHUNK, D), BF16),
                pltpu.VMEM((BATCH, FF), BF16),
                pltpu.VMEM((BATCH * GROUP, HEAD), F32),
                pltpu.VMEM((BATCH * GROUP, HEAD), F32),
                pltpu.VMEM((4, 8, CACHE), BF16),
                pltpu.VMEM((CHUNKS, DEV - 1, CHUNK, OWN), BF16),
                pltpu.VMEM((CHUNKS, CHUNK, OWN), F32),
                pltpu.VMEM((CHUNKS, DEV - 1, CHUNK, OWN), BF16),
                pltpu.VMEM((SUBS, DEV, 16, 128), BF16),
                pltpu.VMEM((LAG + 1, DEV, 16, 128), F32),
                pltpu.VMEM((SUBS, DEV - 1, 16, 128), BF16),
                pltpu.VMEM((BATCH, D), BF16),
                dma, dma((RING,)), dma((RING,)), dma((SLOTS, 2)), dma, dma,
                dma((CHUNKS,)), dma((CHUNKS,)), dma((CHUNKS,)), dma((CHUNKS,)),
                dma, dma((SUBS,)), dma, dma((SUBS,)),
            ],
            compiler_params=pltpu.CompilerParams(
                collective_id=0, has_side_effects=True, vmem_limit_bytes=67043328
            ),
            name="layer",
        )(
            x, k_cache.reshape(BATCH, CACHE, HEAD), v_cache.reshape(BATCH, CACHE, HEAD), gain_a.reshape(1, D),
            jnp.asarray(rotary()), wq, wo, gain_m.reshape(1, D), w_gate, w_up, w_down,
        )

    states, cache, columns, rows_of = P("dp", None), P("dp", None, "tp", None), P(None, "tp"), P("tp", None)
    return jax.shard_map(
        step,
        mesh=mesh,
        in_specs=(states, cache, cache, P(None), columns, rows_of, P(None), columns, columns, rows_of),
        out_specs=states,
        check_vma=False,
    )
```
